16 devices in a mesh: rep: 2 (over y, z), data: 8 (over x, core).
Axes of the slice: x: 4, y: 2, z: 1, core: 2. Of those that a mesh axis runs over, the one named last changes fastest.
The devices are a block of a 4x4x8 slice.
Arguments:
- x: bfloat16 [4096, 3072], P(('rep', 'data')), parts along dimension 0
- adapter_id: int32 [4096], P(('rep', 'data')), parts along dimension 0
- dout: bfloat16 [4096, 3072], P(('rep', 'data')), parts along dimension 0
- w_gate: bfloat16 [3072, 8192], replicated
- w_up: bfloat16 [3072, 8192], replicated
- w_down: bfloat16 [8192, 3072], replicated
- a_gate: bfloat16 [128, 3072, 16], P('data')
- b_gate: bfloat16 [128, 16, 8192], P('data')
- a_up: bfloat16 [128, 3072, 16], P('data')
- b_up: bfloat16 [128, 16, 8192], P('data')
- a_down: bfloat16 [128, 8192, 16], P('data')
- b_down: bfloat16 [128, 16, 3072], P('data')
Outputs:
- output 1: bfloat16 [4096, 3072], P(('rep', 'data')), parts along dimension 0
- output 2: bfloat16 [4096, 3072], P(('rep', 'data')), parts along dimension 0
- output 3: float32 [256, 3072, 16], P(('rep', 'data')), parts along dimension 0
- output 4: float32 [256, 16, 8192], P(('rep', 'data')), parts along dimension 0
- output 5: float32 [256, 3072, 16], P(('rep', 'data')), parts along dimension 0
- output 6: float32 [256, 16, 8192], P(('rep', 'data')), parts along dimension 0
- output 7: float32 [256, 8192, 16], P(('rep', 'data')), parts along dimension 0
- output 8: float32 [256, 16, 3072], P(('rep', 'data')), parts along dimension 0
There are 2 independent parts. The reference program is written for one: setup_inputs(seed, part) draws one part's arguments, and reference() takes and returns one part's arrays. A program takes and returns all parts, laid end to end along the dimension named above; an argument that names none is the same for every part.
All inputs are finite; a program needn't handle non-finite values.
Results may differ from the reference program's by a relative error of at most 0.00139.
Values are sent between devices in bfloat16 or wider.
A program may use at most 768 MiB of HBM per device.

```python
import jax
import jax.numpy as jnp
from jax import lax

TOKENS = 256
ADAPTERS = 16
MODEL_DIM = 3072
HIDDEN_DIM = 8192
LORA_RANK = 16
GROUP_SIZE = 8
CAPACITY = 96
LORA_ALPHA = 32
BLOCK_ROWS = 32

PART_TOKENS = TOKENS * GROUP_SIZE
NUM_ADAPTERS = ADAPTERS * GROUP_SIZE
LORA_SCALE = LORA_ALPHA / LORA_RANK


def draw_ids(rand_key):
    key_hot, key_off, key_shift, key_perm = jax.random.split(rand_key, 4)
    hot_owner = jax.random.randint(key_hot, (), 0, GROUP_SIZE)
    start_offset = jax.random.randint(key_off, (), 0, GROUP_SIZE - 1)
    owner_shift = jax.random.randint(key_shift, (GROUP_SIZE,), 0, ADAPTERS)
    spare_rows = TOKENS - CAPACITY
    source_dev = jnp.arange(GROUP_SIZE)[:, None]
    column_idx = jnp.arange(TOKENS)[None, :]
    hot_mask = column_idx < CAPACITY
    hot_local = (source_dev * CAPACITY + column_idx + owner_shift[hot_owner]) % ADAPTERS
    flat_index = start_offset + source_dev * spare_rows + column_idx - CAPACITY
    other_owner = (hot_owner + 1 + flat_index % (GROUP_SIZE - 1)) % GROUP_SIZE
    visit_count = flat_index // (GROUP_SIZE - 1)
    other_local = (visit_count + owner_shift[other_owner]) % ADAPTERS
    owner_ids = jnp.where(hot_mask, hot_owner, other_owner)
    local_ids = jnp.where(hot_mask, hot_local, other_local)
    id_table = owner_ids * ADAPTERS + local_ids
    perm_keys = jax.random.split(key_perm, GROUP_SIZE)
    perm_rows = jax.vmap(lambda perm_key: jax.random.permutation(perm_key, TOKENS))(perm_keys)
    id_table = jnp.take_along_axis(id_table, perm_rows, axis=1)
    return id_table.reshape(-1).astype(jnp.int32)


def normal_bf16(key_one, arr_shape, spread):
    return (jax.random.normal(key_one, arr_shape, jnp.float32) * spread).astype(jnp.bfloat16)


def setup_inputs(seed: int = 0, part: int = 0) -> dict:
    base_key = jax.random.key(seed)
    part_key = jax.random.fold_in(base_key, part)
    shared_keys = jax.random.split(base_key, 9)
    part_keys = jax.random.split(part_key, 3)
    b_std = 0.3 * LORA_RANK ** -0.5 / LORA_SCALE
    d_std = MODEL_DIM ** -0.5
    f_std = HIDDEN_DIM ** -0.5
    return {
        'x': normal_bf16(part_keys[0], (PART_TOKENS, MODEL_DIM), 1.0),
        'adapter_id': draw_ids(part_keys[1]),
        'dout': normal_bf16(part_keys[2], (PART_TOKENS, MODEL_DIM), 1.0),
        'w_gate': normal_bf16(shared_keys[0], (MODEL_DIM, HIDDEN_DIM), d_std),
        'w_up': normal_bf16(shared_keys[1], (MODEL_DIM, HIDDEN_DIM), d_std),
        'w_down': normal_bf16(shared_keys[2], (HIDDEN_DIM, MODEL_DIM), f_std),
        'a_gate': normal_bf16(shared_keys[3], (NUM_ADAPTERS, MODEL_DIM, LORA_RANK), d_std),
        'b_gate': normal_bf16(shared_keys[4], (NUM_ADAPTERS, LORA_RANK, HIDDEN_DIM), b_std),
        'a_up': normal_bf16(shared_keys[5], (NUM_ADAPTERS, MODEL_DIM, LORA_RANK), d_std),
        'b_up': normal_bf16(shared_keys[6], (NUM_ADAPTERS, LORA_RANK, HIDDEN_DIM), b_std),
        'a_down': normal_bf16(shared_keys[7], (NUM_ADAPTERS, HIDDEN_DIM, LORA_RANK), f_std),
        'b_down': normal_bf16(shared_keys[8], (NUM_ADAPTERS, LORA_RANK, MODEL_DIM), b_std),
    }


def bf16_cast(values):
    return values.astype(jnp.bfloat16).astype(jnp.float32)


def reference(x, adapter_id, dout, w_gate, w_up, w_down, a_gate, b_gate, a_up, b_up, a_down, b_down):
    gate_wt = w_gate.astype(jnp.float32)
    up_wt = w_up.astype(jnp.float32)
    down_wt = w_down.astype(jnp.float32)
    model_width = x.shape[1]
    num_blocks = x.shape[0] // BLOCK_ROWS

    def block_step(grad_sums, block_in):
        x_blk, id_blk, dy_blk = block_in
        x_rows = x_blk.astype(jnp.float32)
        dy_rows = dy_blk.astype(jnp.float32)
        ag_rows = a_gate[id_blk].astype(jnp.float32)
        bg_rows = b_gate[id_blk].astype(jnp.float32)
        au_rows = a_up[id_blk].astype(jnp.float32)
        bu_rows = b_up[id_blk].astype(jnp.float32)
        ad_rows = a_down[id_blk].astype(jnp.float32)
        bd_rows = b_down[id_blk].astype(jnp.float32)
        p_gate = bf16_cast(jnp.einsum('td,tdr->tr', x_rows, ag_rows))
        p_up = bf16_cast(jnp.einsum('td,tdr->tr', x_rows, au_rows))
        e_gate = bf16_cast(LORA_SCALE * jnp.einsum('tr,trf->tf', p_gate, bg_rows))
        e_up = bf16_cast(LORA_SCALE * jnp.einsum('tr,trf->tf', p_up, bu_rows))
        gate_pre = jnp.dot(x_rows, gate_wt) + e_gate
        up_pre = jnp.dot(x_rows, up_wt) + e_up
        gate_sig = jax.nn.sigmoid(gate_pre)
        gate_act = gate_pre * gate_sig
        hidden = bf16_cast(gate_act * up_pre)
        p_down = bf16_cast(jnp.einsum('tf,tfr->tr', hidden, ad_rows))
        e_down = bf16_cast(LORA_SCALE * jnp.einsum('tr,trd->td', p_down, bd_rows))
        out_blk = (x_rows + jnp.dot(hidden, down_wt) + e_down).astype(jnp.bfloat16)
        q_down = bf16_cast(LORA_SCALE * jnp.einsum('td,trd->tr', dy_rows, bd_rows))
        dh_lora = bf16_cast(jnp.einsum('tr,tfr->tf', q_down, ad_rows))
        d_hidden = jnp.einsum('td,fd->tf', dy_rows, down_wt) + dh_lora
        d_gate = bf16_cast(d_hidden * up_pre * gate_sig * (1.0 + gate_pre * (1.0 - gate_sig)))
        d_up = bf16_cast(d_hidden * gate_act)
        q_gate = bf16_cast(LORA_SCALE * jnp.einsum('tf,trf->tr', d_gate, bg_rows))
        q_up = bf16_cast(LORA_SCALE * jnp.einsum('tf,trf->tr', d_up, bu_rows))
        dx_lora = bf16_cast(jnp.einsum('tr,tdr->td', q_gate, ag_rows) + jnp.einsum('tr,tdr->td', q_up, au_rows))
        dx_blk = (dy_rows + jnp.einsum('tf,df->td', d_gate, gate_wt) + jnp.einsum('tf,df->td', d_up, up_wt) + dx_lora).astype(jnp.bfloat16)
        updates = (
            jnp.einsum('td,tr->tdr', x_rows, q_gate),
            LORA_SCALE * jnp.einsum('tr,tf->trf', p_gate, d_gate),
            jnp.einsum('td,tr->tdr', x_rows, q_up),
            LORA_SCALE * jnp.einsum('tr,tf->trf', p_up, d_up),
            jnp.einsum('tf,tr->tfr', hidden, q_down),
            LORA_SCALE * jnp.einsum('tr,td->trd', p_down, dy_rows),
        )
        new_sums = tuple(grad_acc.at[id_blk].add(grad_upd) for grad_acc, grad_upd in zip(grad_sums, updates))
        return new_sums, (out_blk, dx_blk)

    init_sums = tuple(jnp.zeros(weight.shape, jnp.float32) for weight in (a_gate, b_gate, a_up, b_up, a_down, b_down))
    blocks_in = (
        x.reshape(num_blocks, BLOCK_ROWS, model_width),
        adapter_id.reshape(num_blocks, BLOCK_ROWS),
        dout.reshape(num_blocks, BLOCK_ROWS, model_width),
    )
    grad_sums, (out_rows, dx_rows) = lax.scan(block_step, init_sums, blocks_in)
    return (out_rows.reshape(-1, model_width), dx_rows.reshape(-1, model_width), grad_sums[0], grad_sums[1], grad_sums[2], grad_sums[3], grad_sums[4], grad_sums[5])
```

```python
import functools

import jax
import jax.numpy as jnp
from jax import lax
from jax.experimental import pallas as pl
from jax.experimental.pallas import tpu as pltpu
from jax.sharding import PartitionSpec as P

ALPHA = 32
LANES = 128
VMEM_LIMIT = 60 * 1024 * 1024


def mm(a, b):
    return lax.dot_general(a, b, (((1,), (0,)), ((), ())), preferred_element_type=jnp.float32)


def mmt(a, b):
    return lax.dot_general(a, b, (((1,), (1,)), ((), ())), preferred_element_type=jnp.float32)


def tmm(a, b):
    return lax.dot_general(a, b, (((0,), (0,)), ((), ())), preferred_element_type=jnp.float32)


def bf(v):
    return v.astype(jnp.bfloat16)


def pack_kernel(cap, slot_ref, x_ref, d_ref, id_ref, *outs):
    dim = x_ref.shape[1]
    tokens = x_ref.shape[0]
    row = lax.broadcasted_iota(jnp.int32, (cap, tokens), 0)
    slot = slot_ref[...]
    for q, out in enumerate(outs):
        pick = jnp.where(slot == row + q * cap, 1.0, 0.0).astype(jnp.bfloat16)
        out[:, :dim] = bf(mm(pick, x_ref[...]))
        out[:, dim:2 * dim] = bf(mm(pick, d_ref[...]))
        out[:, 2 * dim:] = bf(mm(pick, id_ref[...]))


def pack_rows(slot_row, x, d, ids, n, cap):
    tokens, dim = x.shape
    return pl.pallas_call(
        functools.partial(pack_kernel, cap),
        out_shape=[jax.ShapeDtypeStruct((cap, 2 * dim + LANES), jnp.bfloat16)] * n,
        in_specs=[pl.BlockSpec(memory_space=pltpu.VMEM)] * 4,
        out_specs=[pl.BlockSpec(memory_space=pltpu.VMEM)] * n,
        compiler_params=pltpu.CompilerParams(vmem_limit_bytes=VMEM_LIMIT),
        cost_estimate=pl.CostEstimate(flops=2 * n * cap * tokens * 2 * dim, bytes_accessed=4 * dim * (tokens + n * cap), transcendentals=0),
        name="pack",
    )(slot_row, x, d, ids)


def unpack_kernel(n, cap, slot_ref, *refs):
    outs = refs[2 * n:]
    tokens = slot_ref.shape[0]
    col = lax.broadcasted_iota(jnp.int32, (tokens, n * cap), 1)
    pick = jnp.where(slot_ref[...] == col, 1.0, 0.0).astype(jnp.bfloat16)
    for k in range(2):
        rows = jnp.concatenate([r[...] for r in refs[k * n:(k + 1) * n]], axis=0)
        outs[k][...] = bf(mm(pick, rows))


def unpack_rows(slot_col, parts, cap):
    n = len(parts)
    tokens = slot_col.shape[0]
    dim = parts[0].shape[1] // 2
    width = dim // 3
    steps = dim // width
    return pl.pallas_call(
        functools.partial(unpack_kernel, n, cap),
        grid=(steps,),
        out_shape=[jax.ShapeDtypeStruct((tokens, dim), jnp.bfloat16)] * 2,
        in_specs=[pl.BlockSpec((tokens, 1), lambda j: (0, 0))]
        + [pl.BlockSpec((cap, width), lambda j: (0, j))] * n
        + [pl.BlockSpec((cap, width), lambda j: (0, j + steps))] * n,
        out_specs=[pl.BlockSpec((tokens, width), lambda j: (0, j))] * 2,
        compiler_params=pltpu.CompilerParams(vmem_limit_bytes=VMEM_LIMIT),
        cost_estimate=pl.CostEstimate(flops=2 * n * cap * tokens * 2 * dim, bytes_accessed=4 * dim * (tokens + n * cap), transcendentals=0),
        name="unpack",
    )(slot_col, *parts, *parts)


def layer_kernel(nb, scale, rank, *refs):
    bufs = refs[:nb]
    ag, au, bd, wg, wu, wd, bg, bu, ad = refs[nb:nb + 9]
    res = refs[nb + 9:2 * nb + 9]
    h_out, dg_out, du_out, pq = refs[2 * nb + 9:2 * nb + 13]
    xs, ds, acc_o, acc_x, accp, mask = refs[2 * nb + 13:]
    step = pl.program_id(0)
    cap = bufs[0].shape[0]
    dim = xs.shape[1]
    cols = mask.shape[1]

    @pl.when(step == 0)
    def _():
        for i, b in enumerate(bufs):
            rows = pl.ds(i * cap, cap)
            xs[rows, :] = b[:, :dim]
            ds[rows, :] = b[:, dim:2 * dim]
            aid = b[:, 2 * dim:2 * dim + 1].astype(jnp.float32)
            col = (lax.broadcasted_iota(jnp.int32, (cap, cols), 1) // rank + 1).astype(jnp.float32)
            mask[rows, :] = jnp.where(aid == col, 1.0, 0.0)
        keep = mask[...] > 0.5
        pq[0] = bf(jnp.where(keep, mmt(xs[...], ag[...]), 0.0))
        pq[1] = bf(jnp.where(keep, mmt(xs[...], au[...]), 0.0))
        pq[2] = bf(jnp.where(keep, scale * mmt(ds[...], bd[...]), 0.0))
        acc_o[...] = jnp.zeros_like(acc_o)
        acc_x[...] = jnp.zeros_like(acc_x)
        accp[...] = jnp.zeros_like(accp)

    eg = bf(scale * mm(pq[0], bg[...])).astype(jnp.float32)
    eu = bf(scale * mm(pq[1], bu[...])).astype(jnp.float32)
    el = bf(mm(pq[2], ad[...])).astype(jnp.float32)
    g = mm(xs[...], wg[...]) + eg
    u = mm(xs[...], wu[...]) + eu
    dh = mmt(ds[...], wd[...]) + el
    sig = jax.nn.sigmoid(g)
    act = g * sig
    h = bf(act * u)
    dg = bf(dh * u * sig * (1.0 + g * (1.0 - sig)))
    du = bf(dh * act)
    h_out[...] = h
    dg_out[...] = dg
    du_out[...] = du
    acc_o[...] += mm(h, wd[...])
    acc_x[...] += mmt(dg, wg[...]) + mmt(du, wu[...])
    accp[0] += mmt(h, ad[...])
    accp[1] += mmt(dg, bg[...])
    accp[2] += mmt(du, bu[...])

    @pl.when(step == pl.num_programs(0) - 1)
    def _():
        keep = mask[...] > 0.5
        pd = bf(jnp.where(keep, accp[0], 0.0))
        qg = bf(jnp.where(keep, scale * accp[1], 0.0))
        qu = bf(jnp.where(keep, scale * accp[2], 0.0))
        pq[3] = pd
        pq[4] = qg
        pq[5] = qu
        ed = bf(scale * mm(pd, bd[...])).astype(jnp.float32)
        out = bf(xs[...].astype(jnp.float32) + acc_o[...] + ed)
        dl = bf(mm(qg, ag[...]) + mm(qu, au[...])).astype(jnp.float32)
        dx = bf(ds[...].astype(jnp.float32) + acc_x[...] + dl)
        for i, r in enumerate(res):
            r[:, :dim] = out[i * cap:(i + 1) * cap]
            r[:, dim:] = dx[i * cap:(i + 1) * cap]


def layer(bufs, ag, au, bd, wg, wu, wd, bg, bu, ad, rank, tile, name):
    nb = len(bufs)
    cap = bufs[0].shape[0]
    rows = nb * cap
    dim, hid = wg.shape
    cols = ag.shape[0]
    once = pl.Buffered(1)
    fixed = lambda shape: pl.BlockSpec(shape, lambda f: (0,) * len(shape), pipeline_mode=once)
    flops = 2 * rows * (6 * dim * hid + 6 * cols * (dim + hid))
    byts = 2 * (3 * dim * hid + 3 * cols * (dim + hid) + rows * (4 * dim + 3 * hid))
    out = pl.pallas_call(
        functools.partial(layer_kernel, nb, ALPHA / rank, rank),
        grid=(hid // tile,),
        out_shape=[jax.ShapeDtypeStruct((cap, 2 * dim), jnp.bfloat16)] * nb
        + [jax.ShapeDtypeStruct((rows, hid), jnp.bfloat16)] * 3
        + [jax.ShapeDtypeStruct((6, rows, cols), jnp.bfloat16)],
        in_specs=[fixed((cap, 2 * dim + LANES))] * nb
        + [fixed((cols, dim))] * 3
        + [pl.BlockSpec((dim, tile), lambda f: (0, f))] * 2
        + [pl.BlockSpec((tile, dim), lambda f: (f, 0))]
        + [pl.BlockSpec((cols, tile), lambda f: (0, f))] * 3,
        out_specs=[fixed((cap, 2 * dim))] * nb
        + [pl.BlockSpec((rows, tile), lambda f: (0, f))] * 3
        + [fixed((6, rows, cols))],
        scratch_shapes=[
            pltpu.VMEM((rows, dim), jnp.bfloat16),
            pltpu.VMEM((rows, dim), jnp.bfloat16),
            pltpu.VMEM((rows, dim), jnp.float32),
            pltpu.VMEM((rows, dim), jnp.float32),
            pltpu.VMEM((3, rows, cols), jnp.float32),
            pltpu.VMEM((rows, cols), jnp.float32),
        ],
        compiler_params=pltpu.CompilerParams(vmem_limit_bytes=VMEM_LIMIT),
        cost_estimate=pl.CostEstimate(flops=flops, bytes_accessed=byts, transcendentals=rows * hid),
        name=name,
    )(*bufs, ag, au, bd, wg, wu, wd, bg, bu, ad)
    return out[:nb], out[nb:nb + 3], out[nb + 3]


def grad_f_kernel(ns, scale, *refs):
    pqs = refs[:ns]
    hs, dgs, dus = refs[ns:2 * ns], refs[2 * ns:3 * ns], refs[3 * ns:4 * ns]
    gbg, gbu, gad = refs[4 * ns:]
    cat = lambda vs: jnp.concatenate(vs, axis=0)
    gbg[...] = scale * tmm(cat([p[0] for p in pqs]), cat([r[...] for r in dgs]))
    gbu[...] = scale * tmm(cat([p[1] for p in pqs]), cat([r[...] for r in dus]))
    gad[...] = tmm(cat([p[2] for p in pqs]), cat([r[...] for r in hs]))


def grad_f(pqs, hs, dgs, dus, scale, tile):
    ns = len(pqs)
    cols = pqs[0].shape[2]
    hid = hs[0].shape[1]
    rows = [p.shape[1] for p in pqs]
    return pl.pallas_call(
        functools.partial(grad_f_kernel, ns, scale),
        grid=(hid // tile,),
        out_shape=[jax.ShapeDtypeStruct((cols, hid), jnp.float32)] * 3,
        in_specs=[pl.BlockSpec((6, m, cols), lambda f: (0, 0, 0)) for m in rows]
        + [pl.BlockSpec((m, tile), lambda f: (0, f)) for m in rows] * 3,
        out_specs=[pl.BlockSpec((cols, tile), lambda f: (0, f))] * 3,
        compiler_params=pltpu.CompilerParams(vmem_limit_bytes=VMEM_LIMIT),
        cost_estimate=pl.CostEstimate(flops=6 * cols * sum(rows) * hid, bytes_accessed=6 * hid * (sum(rows) + 2 * cols), transcendentals=0),
        name="grad_hidden",
    )(*pqs, *hs, *dgs, *dus)


def grad_d_kernel(ns, nb, scale, *refs):
    pqs = refs[:ns]
    xs, ds = refs[ns:ns + nb], refs[ns + nb:ns + 2 * nb]
    gag, gau, gbd = refs[ns + 2 * nb:]
    cat = lambda vs: jnp.concatenate(vs, axis=0)
    x = cat([r[...] for r in xs])
    gag[...] = tmm(cat([p[4] for p in pqs]), x)
    gau[...] = tmm(cat([p[5] for p in pqs]), x)
    gbd[...] = scale * tmm(cat([p[3] for p in pqs]), cat([r[...] for r in ds]))


def grad_d(pqs, bufs, dim, scale, tile):
    ns, nb = len(pqs), len(bufs)
    cols = pqs[0].shape[2]
    cap = bufs[0].shape[0]
    steps = dim // tile
    rows = [p.shape[1] for p in pqs]
    return pl.pallas_call(
        functools.partial(grad_d_kernel, ns, nb, scale),
        grid=(steps,),
        out_shape=[jax.ShapeDtypeStruct((cols, dim), jnp.float32)] * 3,
        in_specs=[pl.BlockSpec((6, m, cols), lambda f: (0, 0, 0)) for m in rows]
        + [pl.BlockSpec((cap, tile), lambda f: (0, f))] * nb
        + [pl.BlockSpec((cap, tile), lambda f: (0, f + steps))] * nb,
        out_specs=[pl.BlockSpec((cols, tile), lambda f: (0, f))] * 3,
        compiler_params=pltpu.CompilerParams(vmem_limit_bytes=VMEM_LIMIT),
        cost_estimate=pl.CostEstimate(flops=6 * cols * sum(rows) * dim, bytes_accessed=4 * dim * (sum(rows) + 3 * cols), transcendentals=0),
        name="grad_model",
    )(*pqs, *bufs, *bufs)


def solution(mesh):
    n = mesh.shape['data']
    chips = n // 2
    tok_spec = P(('rep', 'data'), None)
    id_spec = P(('rep', 'data'))
    full_spec = P(None, None)
    own_spec = P('data', None, None)
    grad_spec = P(('rep', 'data'), None, None)
    hops = [0, 1, chips - 1] + list(range(2, chips - 1))
    place = [hops.index(r) for r in range(chips)]

    def there(r, b):
        return [(i, (i // 2 + r) % chips * 2 + (i % 2 ^ b)) for i in range(n)]

    def send(v, r, b):
        return v if r == 0 and b == 0 else lax.ppermute(v, 'data', there(r, b))

    def back(v, r, b):
        return v if r == 0 and b == 0 else lax.ppermute(v, 'data', [(d, s) for s, d in there(r, b)])

    def device_fn(x, ids, dy, w_gate, w_up, w_down, a_gate, b_gate, a_up, b_up, a_down, b_down):
        tokens, dim = x.shape
        hid = w_gate.shape[1]
        n_local, _, rank = a_gate.shape
        cols = n_local * rank
        scale = ALPHA / rank
        cap = ((3 * tokens + 8 * n - 1) // (8 * n)) * 8
        me = lax.axis_index('data')

        ag = a_gate.transpose(0, 2, 1).reshape(cols, dim)
        au = a_up.transpose(0, 2, 1).reshape(cols, dim)
        ad = a_down.transpose(0, 2, 1).reshape(cols, hid)
        bg = b_gate.reshape(cols, hid)
        bu = b_up.reshape(cols, hid)
        bd = b_down.reshape(cols, dim)

        owner = ids // n_local
        rel = (owner // 2 - me // 2) % chips
        pos = jnp.zeros_like(rel)
        for r in range(chips):
            pos = jnp.where(rel == r, place[r], pos)
        pos = 2 * pos + (owner % 2 + me % 2) % 2
        t = jnp.arange(tokens, dtype=jnp.int32)
        before = (owner[:, None] == owner[None, :]) & (t[None, :] < t[:, None])
        slot = pos * cap + jnp.sum(before.astype(jnp.int32), axis=1)
        idc = jnp.broadcast_to((ids % n_local + 1)[:, None], (tokens, LANES)).astype(jnp.bfloat16)

        packed = pack_rows(slot[None, :], x, dy, idc, n, cap)

        def stage(bufs, name):
            return layer(bufs, ag, au, bd, w_gate, w_up, w_down, bg, bu, ad, rank, 512, name)

        groups = [[0], [1, 2], list(range(3, chips))]
        got = [None] * n
        for p in range(6):
            got[p] = send(packed[p], hops[p // 2], p % 2)
        res0, hid0, pq0 = stage(got[0:2], "layer_own")
        late, _ = lax.optimization_barrier((tuple(packed[6:]), pq0))
        for p in range(6, n):
            got[p] = send(late[p - 6], hops[p // 2], p % 2)
        res1, hid1, pq1 = stage(got[2:6], "layer_near")
        res2, hid2, pq2 = stage(got[6:], "layer_far")
        res = list(res0) + list(res1) + list(res2)
        parts = [back(res[p], hops[p // 2], p % 2) for p in range(n)]

        pqs = [pq0, pq1, pq2]
        hids = [hid0, hid1, hid2]
        gbg, gbu, gad = grad_f(pqs, [v[0] for v in hids], [v[1] for v in hids], [v[2] for v in hids], scale, 512)
        gag, gau, gbd = grad_d(pqs, got, dim, scale, 512)
        out, dx = unpack_rows(slot[:, None], parts, cap)

        def as_a(v):
            return v.reshape(n_local, rank, v.shape[1]).transpose(0, 2, 1)

        def as_b(v):
            return v.reshape(n_local, rank, v.shape[1])

        return out, dx, as_a(gag), as_b(gbg), as_a(gau), as_b(gbu), as_a(gad), as_b(gbd)

    return jax.shard_map(
        device_fn,
        mesh=mesh,
        in_specs=(tok_spec, id_spec, tok_spec, full_spec, full_spec, full_spec, own_spec, own_spec, own_spec, own_spec, own_spec, own_spec),
        out_specs=(tok_spec, tok_spec, grad_spec, grad_spec, grad_spec, grad_spec, grad_spec, grad_spec),
        check_vma=False,
    )
```
